32 devices in a mesh: ep: 8 (over z, y), dp: 4 (over x, core).
Axes of the slice: x: 2, y: 2, z: 4, core: 2. Of those that a mesh axis runs over, the one named last changes fastest.
Arguments:
- tokens: bfloat16 [512, 7168], P(('ep', 'dp')), may hold values from -6 to 6
- routes: int32 [512, 2], P(('ep', 'dp')), may hold values from 0 to 7, all different within a row; in each aligned block of 16 rows (0 to 15, 16 to 31, ...) at most 8 rows name the same one
- route_logits: float32 [512, 2], P(('ep', 'dp')), may hold values from -6 to 6
- gate_weight: bfloat16 [8, 7168, 2048], P('ep', None, 'dp'), may hold values from -0.0625 to 0.0625
- up_weight: bfloat16 [8, 7168, 2048], P('ep', None, 'dp'), may hold values from -0.0625 to 0.0625
- down_weight: bfloat16 [8, 2048, 7168], P('ep', 'dp'), may hold values from -0.125 to 0.125
Outputs:
- moe_output: bfloat16 [512, 7168], P(('ep', 'dp'))
- expert_load: float32 [8], P('ep')
The draws below stay inside these ranges and needn't reach their ends.
Inputs may be any that keep to these rules, and one draw needn't show every extreme that they name: `routes`: each row names 2 different experts. Within the rows of one device (aligned blocks of 16 rows) no expert is named more than 8 times, and in every draw some expert is named exactly 8 times there; every expert is named somewhere.
All inputs are finite; a program needn't handle non-finite values.
Results may differ from the reference program's by a relative error of at most 0.012.
Values may be sent and summed in bfloat16 or wider, within the bound.
A program may use at most 128 MiB of HBM per device.

```python
import math
import jax
import jax.numpy as jnp
import numpy as np
from jax import lax

D = 7168
FF = 2048
TOK_DEV = 16
EXPERTS = 8
TOP = 2
CAP = 8
TOKENS = 512
N_EP = 8
N_DP = 4


def levels(key, extent, split, smallest, high):
    level, own = 1.0, jax.random.fold_in(key, 6)
    for dim, shards_of in split:
        heights = jnp.exp(jax.random.uniform(jax.random.fold_in(own, dim), (shards_of,), jnp.float32, smallest / len(split), high / len(split)))
        level = level * jnp.repeat(heights, extent[dim] // shards_of).reshape([-1 if axis == dim else 1 for axis in range(len(extent))])
    return level


def assign_block(rng, own, number, rows, amount, top, bound, slope):
    sequence = jax.random.permutation(rng, amount)
    packed, common = load_shares(amount, rows * top, bound, slope, True), load_shares(amount, rows * top, bound, slope, False)
    places = jnp.arange(amount)

    def named(tallies, turn):
        used = int((tallies > 0).sum())
        fixed = max(1, used // 4)
        passed = fixed + (places - fixed + turn * (used - fixed)) % max(1, amount - fixed)
        return jnp.zeros((amount,), jnp.int32).at[sequence[jnp.where(places < fixed, places, passed)]].set(jnp.asarray(tallies, jnp.int32))

    tallies = jnp.where(number % 4 == 0, named(packed, number // 4), named(common, number - number // 4 - 1))
    mixed = jax.random.permutation(jax.random.fold_in(own, 3), amount)
    source_of, receiver = mixed[0:amount // 2 * 2:2], mixed[1:amount // 2 * 2:2]
    margin = jnp.minimum(tallies[source_of] - 1, bound - tallies[receiver]) // 2
    margin = jnp.where((source_of == sequence[0]) | (receiver == sequence[0]) | (tallies[receiver] == 0), 0, jnp.maximum(margin, 0))
    passed = jax.random.randint(jax.random.fold_in(own, 4), (amount // 2,), 0, 1 << 20) % (margin + 1)
    tallies = tallies.at[source_of].add(-passed).at[receiver].add(passed)
    items = jnp.searchsorted(jnp.cumsum(tallies), jnp.arange(rows * top), side="right").astype(jnp.int32)
    table = items.reshape(top, rows).T
    table = table[jax.random.permutation(jax.random.fold_in(own, 1), rows)]
    turn = jax.random.randint(jax.random.fold_in(own, 2), (rows, 1), 0, top)
    return jnp.take_along_axis(table, (jnp.arange(top)[None, :] + turn) % top, axis=1)


def load_shares(amount, total, most, lean, full):
    portions = [(1 << 20) // math.isqrt(standing ** lean) + 1 for standing in range(1, amount + 1)]
    largest = most if full else min(most, max(-(-total // amount), total * portions[0] // sum(portions)))
    least = 1 if total - largest >= amount - 1 else 0
    given, rest = [largest] + [least] * (amount - 1), total - largest - least * (amount - 1)
    while rest > 0:
        movable = [i for i in range(1, amount) if given[i] < largest] or [i for i in range(1, amount) if given[i] < most]
        whole, left = sum([portions[i] for i in movable]), rest
        for i in movable:
            extra = min(most - given[i], max(1, left * portions[i] // whole), rest)
            given[i] = given[i] + extra
            rest = rest - extra
    return np.array(given)


def scatter_about(rng, shape, spread, limit, split=(), held_as=jnp.bfloat16):
    loudness = levels(rng, shape, split, -0.22, 0.18) if split else 1.0
    drawn = jax.random.normal(rng, shape, jnp.float32) * spread * loudness
    return jnp.minimum(jnp.maximum(drawn, -limit), limit).astype(held_as)


def setup_inputs(seed: int = 0) -> dict:
    splits = jax.random.split(jax.random.key(seed), 7)
    tokens = scatter_about(splits[0], (TOKENS, D), 1.0, 6.0, ((0, 32),))
    routes_keys = jax.random.split(jax.random.fold_in(splits[1], 1), TOKENS // TOK_DEV)
    routes_turns = jax.random.permutation(jax.random.fold_in(splits[1], 3), TOKENS // TOK_DEV)
    routes = jax.vmap(lambda own, number: assign_block(jax.random.fold_in(splits[1], 2), own, number, TOK_DEV, EXPERTS, TOP, CAP, 2))(routes_keys, routes_turns).reshape((TOKENS, TOP))
    route_logits = scatter_about(splits[2], (TOKENS, TOP), 1.5, 6.0, ((0, 32),), jnp.float32)
    gate_weight = scatter_about(splits[3], (EXPERTS, D, FF), D ** -0.5, 0.0625, ((0, 8), (2, 4)))
    up_weight = scatter_about(splits[4], (EXPERTS, D, FF), D ** -0.5, 0.0625, ((0, 8), (2, 4)))
    down_weight = scatter_about(splits[5], (EXPERTS, FF, D), FF ** -0.5, 0.125, ((0, 8), (1, 4)))
    return dict(tokens=tokens, routes=routes, route_logits=route_logits, gate_weight=gate_weight, up_weight=up_weight, down_weight=down_weight)


ROUTE_SCALE = 2.5


def reference(tokens, routes, route_logits, gate_weight, up_weight, down_weight):
    device_count = N_EP * N_DP
    per_block = TOK_DEV * TOP
    quarter = FF // N_DP
    flat_routes = routes.reshape(device_count, per_block)
    labels = jnp.arange(EXPERTS, dtype=jnp.int32)
    onehot = (flat_routes[:, :, None] == labels[None, None, :]).astype(jnp.int32)
    slot_ids = jnp.sum((jnp.cumsum(onehot, axis=1) - onehot) * onehot, axis=2)
    expert_count = jnp.sum(onehot, axis=(0, 1)).astype(jnp.float32)
    affinity = jax.nn.sigmoid(route_logits)
    weights = ROUTE_SCALE * affinity / jnp.sum(affinity, axis=1, keepdims=True)
    device_ids = jnp.arange(device_count, dtype=jnp.int32)[:, None]
    token_ids = device_ids * TOK_DEV + jnp.arange(per_block, dtype=jnp.int32)[None, :] // TOP
    position = ((flat_routes * device_count + device_ids) * CAP + slot_ids).reshape(-1).astype(jnp.int32)
    token_table = jnp.zeros((EXPERTS * device_count * CAP,), jnp.int32).at[position].set(token_ids.reshape(-1).astype(jnp.int32))
    weight_table = jnp.zeros((EXPERTS * device_count * CAP,), jnp.float32).at[position].set(weights.reshape(-1))
    token_table = token_table.reshape(EXPERTS, device_count * CAP)
    weight_table = weight_table.reshape(EXPERTS, device_count * CAP)

    def expert_step(running, inputs):
        row_index, slot_weight, gate_w, up_w, down_w = inputs
        row_block = tokens[row_index]
        gate_act = jnp.dot(row_block, gate_w, preferred_element_type=jnp.float32)
        up_act = jnp.dot(row_block, up_w, preferred_element_type=jnp.float32)
        hidden = (jax.nn.silu(gate_act) * up_act).astype(jnp.bfloat16)
        pieces = []
        for index_q in range(N_DP):
            lower = index_q * quarter
            piece = jnp.dot(hidden[:, lower:lower + quarter], down_w[lower:lower + quarter], preferred_element_type=jnp.float32)
            pieces.append(piece.astype(jnp.bfloat16))
        pieces = lax.optimization_barrier(pieces)
        expert_out = pieces[0].astype(jnp.float32)
        for piece in pieces[1:]:
            expert_out = expert_out + piece.astype(jnp.float32)
        return running.at[row_index].add(expert_out * slot_weight[:, None]), None

    running, _ = lax.scan(expert_step, jnp.zeros((TOKENS, D), jnp.float32), (token_table, weight_table, gate_weight, up_weight, down_weight))
    moe_output = running.astype(jnp.bfloat16)
    mean_count = float(TOK_DEV * N_DP * TOP)
    expert_load = expert_count / mean_count
    return moe_output, expert_load
```

```python
import functools

import jax
import jax.numpy as jnp
from jax import lax
from jax.experimental import pallas as pl
from jax.experimental.pallas import tpu as pltpu
from jax.sharding import PartitionSpec as P

ROUTE_SCALE = 2.5
PRECISE = lax.Precision.HIGHEST


def assignment_slots(flat_routes, experts):
    labels = jnp.arange(experts, dtype=jnp.int32)
    onehot = (flat_routes[:, :, None] == labels[None, None, :]).astype(jnp.int32)
    before = jnp.cumsum(onehot, axis=1) - onehot
    return (jnp.sum(before * onehot, axis=2), jnp.sum(onehot, axis=1))


def pack(members, flat_routes, slot_ids, experts, capacity, top_k):
    blocks, per_block = flat_routes.shape
    tok_dev = per_block // top_k
    member = jnp.arange(blocks, dtype=jnp.int32)[:, None]
    target = ((member * experts + flat_routes) * capacity + slot_ids).reshape(-1)
    source = (member * tok_dev + jnp.arange(per_block, dtype=jnp.int32)[None, :] // top_k).reshape(
        -1
    )
    placing = (
        jnp.arange(blocks * experts * capacity, dtype=jnp.int32)[:, None] == target[None, :]
    ).astype(jnp.bfloat16)
    owners = (source[:, None] == jnp.arange(blocks * tok_dev, dtype=jnp.int32)[None, :]).astype(
        jnp.bfloat16
    )
    picker = jnp.dot(placing, owners, preferred_element_type=jnp.float32).astype(jnp.bfloat16)
    filled = jnp.dot(picker, members, preferred_element_type=jnp.float32).astype(jnp.bfloat16)
    return filled.reshape(blocks, experts, capacity, members.shape[1])


def expert_rows(row_block, gate_w, up_w, down_w):
    gate_act = jnp.dot(row_block, gate_w, preferred_element_type=jnp.float32)
    up_act = jnp.dot(row_block, up_w, preferred_element_type=jnp.float32)
    hidden = (jax.nn.silu(gate_act) * up_act).astype(jnp.bfloat16)
    return jnp.dot(hidden, down_w, preferred_element_type=jnp.float32)


def on_device(tokens, routes, route_logits, gate_weight, up_weight, down_weight):
    tok_dev, top_k = routes.shape
    model_width = tokens.shape[1]
    experts = lax.axis_size("ep")
    groups = lax.axis_size("dp")
    capacity = min(tok_dev // 2, 2 * tok_dev * top_k // experts)
    per_block = tok_dev * top_k
    gate_w = gate_weight[0]
    up_w = up_weight[0]
    down_w = down_weight[0]
    own_flat = routes.reshape(1, per_block)
    own_slots, own_counts = assignment_slots(own_flat, experts)
    buffer = pack(tokens, own_flat, own_slots, experts, capacity, top_k)
    received = lax.all_to_all(buffer, "ep", split_axis=1, concat_axis=1, tiled=True)
    partial_value = expert_rows(
        lax.all_gather(received.reshape(-1, model_width), "dp", axis=0, tiled=True),
        gate_w,
        up_w,
        down_w,
    )
    shares = lax.psum_scatter(
        partial_value.astype(jnp.bfloat16), "dp", scatter_dimension=0, tiled=True
    ).astype(jnp.float32)
    returned = lax.all_to_all(
        shares.reshape(experts, capacity, model_width).astype(jnp.bfloat16),
        "ep",
        split_axis=0,
        concat_axis=0,
        tiled=True,
    ).astype(jnp.float32)
    affinity = jax.nn.sigmoid(route_logits)
    weights = (ROUTE_SCALE * affinity / jnp.sum(affinity, axis=1, keepdims=True)).reshape(-1)
    own_target = own_flat[0] * capacity + own_slots[0]
    spread = jnp.where(
        own_target[:, None] == jnp.arange(experts * capacity, dtype=jnp.int32)[None, :],
        weights[:, None],
        0.0,
    )
    owners = (
        jnp.arange(tok_dev, dtype=jnp.int32)[:, None]
        == jnp.arange(per_block, dtype=jnp.int32)[None, :] // top_k
    ).astype(jnp.float32)
    combine = jnp.dot(owners, spread, precision=PRECISE)
    moe_output = jnp.dot(
        combine, returned.reshape(experts * capacity, model_width), precision=PRECISE
    ).astype(jnp.bfloat16)
    local_counts = own_counts[0].astype(jnp.float32)
    whole = lax.psum(local_counts, ("ep", "dp"))
    expert_count = lax.dynamic_slice_in_dim(whole, lax.axis_index("ep"), 1)
    mean_count = float(tok_dev * groups * top_k)
    expert_load = expert_count / mean_count
    return (moe_output, expert_load)


MESH = pl.DeviceIdType.MESH
WINDOW = 6
X_LAG = 3
C_LAG = 2
H_LAG = 2
B_LAG = 6
R_LAG = 3


def chunk_count(width):
    for count in (14, 7, 8, 4, 2):
        if width % (count * 128) == 0:
            return count
    return 1


def remote(src, dst, send, recv, ep, dp):
    return pltpu.make_async_remote_copy(
        src_ref=src,
        dst_ref=dst,
        send_sem=send,
        recv_sem=recv,
        device_id={"ep": ep, "dp": dp},
        device_id_type=MESH,
    )


def fused_kernel(
    E, G, cap, nc, dc, mean_count,
    routes_hbm, logits_hbm, tokens_hbm, wg_hbm, wu_hbm, wd_hbm,
    out, load, routes_t, logits_t, tokens,
    wg, wu, wd, slots, rows, acc_g, acc_u, hidden, part, a_recv, b_send, b_recv, r_send, r_recv,
    combine, cnt_send, cnt_recv, dcnt_send, dcnt_recv,
    in_sem, w_sem, s1_send, s1_recv, x_send, x_recv, c_send, c_recv,
    ra_send, ra_recv, rb_send, rb_recv, rr_send, rr_recv,
    n_send, n_recv, nd_send, nd_recv,
):
    me = lax.axis_index("ep")
    dp = lax.axis_index("dp")
    hi = dp // 2
    lo = dp % 2
    px = (1 - hi) * 2 + lo
    pc = hi * 2 + (1 - lo)
    top, tok = routes_hbm.shape
    n_slots = E * cap

    def landed(ref, sem):
        pltpu.make_async_copy(ref, ref, sem).wait()

    def peers(body):
        def step(k, carry):
            body(lax.rem(me + k, E))
            return carry

        lax.fori_loop(1, E, step, 0)

    barrier = pltpu.get_barrier_semaphore()
    peers(lambda e: pl.semaphore_signal(
        barrier, inc=1, device_id={"ep": e, "dp": dp}, device_id_type=MESH))
    pl.semaphore_signal(barrier, inc=1, device_id={"ep": me, "dp": px}, device_id_type=MESH)
    pl.semaphore_signal(barrier, inc=1, device_id={"ep": me, "dp": pc}, device_id_type=MESH)

    inputs = [
        pltpu.make_async_copy(src, dst, in_sem.at[i])
        for i, (src, dst) in enumerate(
            ((routes_hbm, routes_t), (logits_hbm, logits_t), (tokens_hbm, tokens)))
    ]
    for copy in inputs:
        copy.start()

    def weight_copies(c):
        cols = pl.ds(pl.multiple_of(c * dc, 128), dc)
        return (
            pltpu.make_async_copy(wg_hbm.at[0, cols], wg.at[c], w_sem.at[0, c]),
            pltpu.make_async_copy(wu_hbm.at[0, cols], wu.at[c], w_sem.at[1, c]),
            pltpu.make_async_copy(wd_hbm.at[0, :, cols], wd.at[c], w_sem.at[2, c]),
        )

    def start_weights(c, carry):
        copies = weight_copies(c)
        copies[0].start()
        copies[1].start()
        return carry

    def start_down(c, carry):
        weight_copies(c)[2].start()
        return carry

    lax.fori_loop(0, nc, start_weights, 0)
    lax.fori_loop(0, nc, start_down, 0)

    for copy in inputs:
        copy.wait()
    slot_row = lax.broadcasted_iota(jnp.int32, (n_slots, tok), 0)
    named = jnp.zeros((n_slots, tok), jnp.float32)
    for k in range(top):
        named = named + jnp.where(routes_t[k:k + 1, :] == slot_row // cap, 1.0, 0.0)
    earlier = jnp.where(
        lax.broadcasted_iota(jnp.int32, (tok, tok), 0)
        < lax.broadcasted_iota(jnp.int32, (tok, tok), 1), 1.0, 0.0)
    before = jnp.dot(named, earlier, preferred_element_type=jnp.float32)
    placed = before == (slot_row % cap).astype(jnp.float32)
    picker = jnp.where(placed, named, 0.0).astype(jnp.bfloat16)
    counted = jnp.sum(named, axis=1, keepdims=True)
    cnt_send[...] = jnp.broadcast_to(counted, (n_slots, 128)).reshape(E, cap, 128)

    def pack_chunk(c, carry):
        cols = pl.ds(pl.multiple_of(c * dc, 128), dc)
        filled = jnp.dot(picker, tokens[:, cols], preferred_element_type=jnp.float32)
        slots[c] = filled.reshape(E, cap, dc).astype(jnp.bfloat16)
        rows[c, dp, me] = slots[c, me]
        return carry

    lax.fori_loop(0, nc, pack_chunk, 0)
    cnt_recv[me] = cnt_send[me]

    def first(c, src, dst_e):
        return remote(slots.at[c, dst_e], rows.at[c, dp, src],
                      s1_send, s1_recv.at[c], dst_e, dp)

    def counts(src, dst_e):
        return remote(cnt_send.at[dst_e], cnt_recv.at[src],
                      n_send, n_recv, dst_e, dp)

    pl.semaphore_wait(barrier, E + 1)

    def send_first(c, carry):
        peers(lambda e: first(c, me, e).start())
        return carry

    lax.fori_loop(0, min(WINDOW, nc), send_first, 0)
    peers(lambda e: counts(me, e).start())

    affinity = jax.nn.sigmoid(logits_t[...])
    weights = ROUTE_SCALE * affinity / jnp.sum(affinity, axis=0, keepdims=True)
    spread = jnp.zeros((n_slots, tok), jnp.float32)
    for k in range(top):
        hit = routes_t[k:k + 1, :] == slot_row // cap
        spread = spread + jnp.where(hit, weights[k:k + 1, :], 0.0)
    spread = jnp.where(placed, spread, 0.0)
    coarse = spread.astype(jnp.bfloat16)
    rest = spread - coarse.astype(jnp.float32)
    middle = rest.astype(jnp.bfloat16)
    fine = (rest - middle.astype(jnp.float32)).astype(jnp.bfloat16)
    same = jnp.where(
        lax.broadcasted_iota(jnp.int32, (tok, tok), 0)
        == lax.broadcasted_iota(jnp.int32, (tok, tok), 1), 1.0, 0.0).astype(jnp.bfloat16)
    for i, piece in enumerate((coarse, middle, fine)):
        turned = lax.dot_general(
            same, piece, (((1,), (1,)), ((), ())), preferred_element_type=jnp.float32)
        combine[i * tok:(i + 1) * tok] = turned.astype(jnp.bfloat16)

    acc_g[...] = jnp.zeros_like(acc_g)
    acc_u[...] = jnp.zeros_like(acc_u)

    def across(c, who):
        return remote(rows.at[c, who], rows.at[c, who], x_send, x_recv.at[c], me, px)

    def beside(c, i, who):
        return remote(rows.at[c, who], rows.at[c, who],
                      c_send, c_recv.at[c], me, pc)

    def forward(s, carry):
        @pl.when(s < nc)
        def _():
            landed(rows.at[s, dp, 0:E - 1], s1_recv.at[s])
            across(s, dp).start()
            beside(s, 0, dp).start()

        @pl.when(s + WINDOW < nc)
        def _():
            send_first(s + WINDOW, 0)

        @pl.when((s >= X_LAG) & (s < nc + X_LAG))
        def _():
            c = s - X_LAG
            across(c, px).wait_recv()
            beside(c, 1, px).start()

        @pl.when(s >= X_LAG + C_LAG)
        def _():
            c = s - X_LAG - C_LAG
            landed(rows.at[c, 0:2], c_recv.at[c])
            copies = weight_copies(c)
            copies[0].wait()
            copies[1].wait()
            x = rows[c].astype(jnp.float32).reshape(G * n_slots, dc).astype(jnp.bfloat16)
            acc_g[...] += jnp.dot(x, wg[c], preferred_element_type=jnp.float32)
            acc_u[...] += jnp.dot(x, wu[c], preferred_element_type=jnp.float32)

        return carry

    lax.fori_loop(0, nc + X_LAG + C_LAG, forward, 0)
    landed(cnt_recv.at[0:E - 1], n_recv)
    mine = cnt_recv[0]
    for e in range(1, E):
        mine = mine + cnt_recv[e]
    dcnt_send[...] = mine
    for i in range(1, G):
        remote(dcnt_send, dcnt_recv.at[i - 1], nd_send, nd_recv, me, lax.rem(dp + i, G)).start()
    gate = acc_g[...]
    hidden[...] = (gate / (1.0 + jnp.exp(-gate)) * acc_u[...]).astype(jnp.bfloat16)

    def half(c, h):
        return remote(part.at[c, h * 2 + (1 - lo)], a_recv.at[c, h],
                      ra_send, ra_recv.at[c, h], me, pc)

    def quarter(c):
        return remote(b_send.at[c], b_recv.at[c], rb_send, rb_recv.at[c], me, px)

    def back(c, src, dst_e):
        return remote(r_send.at[c, dst_e], r_recv.at[c, src],
                      rr_send, rr_recv.at[c], dst_e, dp)

    def wide(value):
        return value.astype(jnp.float32)

    def backward(s, carry):
        @pl.when(s < nc)
        def _():
            weight_copies(s)[2].wait()
            p = jnp.dot(hidden[...], wd[s], preferred_element_type=jnp.float32)
            part[s] = p.reshape(G, E, cap, dc).astype(jnp.bfloat16)
            half(s, 1 - hi).start()
            half(s, hi).start()

        @pl.when((s >= H_LAG) & (s < nc + H_LAG))
        def _():
            c = s - H_LAG
            half(c, 1 - hi).wait_recv()
            total = wide(part[c, px]) + wide(a_recv[c, 1 - hi])
            b_send[c] = total.astype(jnp.bfloat16)
            quarter(c).start()

        @pl.when((s >= B_LAG) & (s < nc + B_LAG))
        def _():
            c = s - B_LAG
            half(c, hi).wait_recv()
            quarter(c).wait_recv()
            total = wide(part[c, dp]) + wide(a_recv[c, hi]) + wide(b_recv[c])
            r_send[c] = total.astype(jnp.bfloat16)
            peers(lambda e: back(c, me, e).start())
            r_recv[c, me] = r_send[c, me]

        @pl.when(s >= B_LAG + R_LAG)
        def _():
            c = s - B_LAG - R_LAG
            landed(r_recv.at[c, 0:E - 1], rr_recv.at[c])
            got = r_recv[c].astype(jnp.float32).reshape(n_slots, dc).astype(jnp.bfloat16)
            mixed = jnp.dot(combine[...], got, preferred_element_type=jnp.float32)
            total = mixed[0:tok] + mixed[tok:2 * tok] + mixed[2 * tok:3 * tok]
            out[:, pl.ds(pl.multiple_of(c * dc, 128), dc)] = total.astype(jnp.bfloat16)

        return carry

    lax.fori_loop(0, nc + B_LAG + R_LAG, backward, 0)

    landed(dcnt_recv.at[0:G - 1], nd_recv)
    mine = dcnt_send[...]
    for i in range(G - 1):
        mine = mine + dcnt_recv[i]
    load[...] = mine[0:1, :] / mean_count

    landed(cnt_recv.at[0:E - 1], n_send)
    landed(dcnt_recv.at[0:G - 1], nd_send)
    landed(slots.at[:, 0:E - 1], s1_send)
    landed(b_send, x_send)
    landed(a_recv, c_send)
    landed(a_recv, ra_send)
    landed(b_send, rb_send)
    landed(r_send.at[:, 0:E - 1], rr_send)


def fused_device(tokens, routes, route_logits, gate_weight, up_weight, down_weight):
    tok_dev, top_k = routes.shape
    width = tokens.shape[1]
    units = gate_weight.shape[2]
    E = lax.axis_size("ep")
    G = lax.axis_size("dp")
    cap = min(tok_dev // 2, 2 * tok_dev * top_k // E)
    nc = chunk_count(width)
    dc = width // nc
    bf, f32 = jnp.bfloat16, jnp.float32
    dma = pltpu.SemaphoreType.DMA
    vmem = pl.BlockSpec(memory_space=pltpu.VMEM)
    anywhere = pl.BlockSpec(memory_space=pl.ANY)
    rows = G * E * cap
    moe_output, load = pl.pallas_call(
        functools.partial(fused_kernel, E, G, cap, nc, dc, float(tok_dev * G * top_k)),
        out_shape=(
            jax.ShapeDtypeStruct((tok_dev, width), bf),
            jax.ShapeDtypeStruct((1, 128), f32),
        ),
        in_specs=[anywhere] * 6,
        out_specs=(vmem, vmem),
        scratch_shapes=[
            pltpu.VMEM((top_k, tok_dev), jnp.int32),
            pltpu.VMEM((top_k, tok_dev), f32),
            pltpu.VMEM((tok_dev, width), bf),
            pltpu.VMEM((nc, dc, units), bf),
            pltpu.VMEM((nc, dc, units), bf),
            pltpu.VMEM((nc, units, dc), bf),
            pltpu.VMEM((nc, E, cap, dc), bf),
            pltpu.VMEM((nc, G, E, cap, dc), bf),
            pltpu.VMEM((rows, units), f32),
            pltpu.VMEM((rows, units), f32),
            pltpu.VMEM((rows, units), bf),
            pltpu.VMEM((nc, G, E, cap, dc), bf),
            pltpu.VMEM((nc, 2, E, cap, dc), bf),
            pltpu.VMEM((nc, E, cap, dc), bf),
            pltpu.VMEM((nc, E, cap, dc), bf),
            pltpu.VMEM((nc, E, cap, dc), bf),
            pltpu.VMEM((nc, E, cap, dc), bf),
            pltpu.VMEM((3 * tok_dev, E * cap), bf),
            pltpu.VMEM((E, cap, 128), f32),
            pltpu.VMEM((E, cap, 128), f32),
            pltpu.VMEM((cap, 128), f32),
            pltpu.VMEM((G - 1, cap, 128), f32),
            dma((3,)),
            dma((3, nc)),
            dma, dma((nc,)),
            dma, dma((nc,)),
            dma, dma((nc,)),
            dma, dma((nc, 2)),
            dma, dma((nc,)),
            dma, dma((nc,)),
            dma, dma,
            dma, dma,
        ],
        compiler_params=pltpu.CompilerParams(
            collective_id=0, has_side_effects=True, vmem_limit_bytes=60 * 2**20
        ),
    )(routes.T, route_logits.T, tokens, gate_weight, up_weight, down_weight)
    return moe_output, load[0, :1]


def fits(mesh):
    return mesh.shape["dp"] == 4 and mesh.shape["ep"] <= 8


def solution(mesh):
    body = fused_device if fits(mesh) else on_device
    return jax.shard_map(
        body,
        mesh=mesh,
        in_specs=(
            P(("ep", "dp"), None),
            P(("ep", "dp"), None),
            P(("ep", "dp"), None),
            P("ep", None, "dp"),
            P("ep", None, "dp"),
            P("ep", "dp", None),
        ),
        out_specs=(P(("ep", "dp"), None), P("ep")),
        check_vma=False,
    )
```

```python
import functools

import jax
import jax.numpy as jnp
from jax import lax
from jax.experimental import pallas as pl
from jax.experimental.pallas import tpu as pltpu
from jax.sharding import PartitionSpec as P

ROUTE_SCALE = 2.5
PRECISE = lax.Precision.HIGHEST


def assignment_slots(flat_routes, experts):
    labels = jnp.arange(experts, dtype=jnp.int32)
    onehot = (flat_routes[:, :, None] == labels[None, None, :]).astype(jnp.int32)
    before = jnp.cumsum(onehot, axis=1) - onehot
    return (jnp.sum(before * onehot, axis=2), jnp.sum(onehot, axis=1))


def pack(members, flat_routes, slot_ids, experts, capacity, top_k):
    blocks, per_block = flat_routes.shape
    tok_dev = per_block // top_k
    member = jnp.arange(blocks, dtype=jnp.int32)[:, None]
    target = ((member * experts + flat_routes) * capacity + slot_ids).reshape(-1)
    source = (member * tok_dev + jnp.arange(per_block, dtype=jnp.int32)[None, :] // top_k).reshape(
        -1
    )
    placing = (
        jnp.arange(blocks * experts * capacity, dtype=jnp.int32)[:, None] == target[None, :]
    ).astype(jnp.bfloat16)
    owners = (source[:, None] == jnp.arange(blocks * tok_dev, dtype=jnp.int32)[None, :]).astype(
        jnp.bfloat16
    )
    picker = jnp.dot(placing, owners, preferred_element_type=jnp.float32).astype(jnp.bfloat16)
    filled = jnp.dot(picker, members, preferred_element_type=jnp.float32).astype(jnp.bfloat16)
    return filled.reshape(blocks, experts, capacity, members.shape[1])


def expert_rows(row_block, gate_w, up_w, down_w):
    gate_act = jnp.dot(row_block, gate_w, preferred_element_type=jnp.float32)
    up_act = jnp.dot(row_block, up_w, preferred_element_type=jnp.float32)
    hidden = (jax.nn.silu(gate_act) * up_act).astype(jnp.bfloat16)
    return jnp.dot(hidden, down_w, preferred_element_type=jnp.float32)


def on_device(tokens, routes, route_logits, gate_weight, up_weight, down_weight):
    tok_dev, top_k = routes.shape
    model_width = tokens.shape[1]
    experts = lax.axis_size("ep")
    groups = lax.axis_size("dp")
    capacity = min(tok_dev // 2, 2 * tok_dev * top_k // experts)
    per_block = tok_dev * top_k
    gate_w = gate_weight[0]
    up_w = up_weight[0]
    down_w = down_weight[0]
    own_flat = routes.reshape(1, per_block)
    own_slots, own_counts = assignment_slots(own_flat, experts)
    buffer = pack(tokens, own_flat, own_slots, experts, capacity, top_k)
    received = lax.all_to_all(buffer, "ep", split_axis=1, concat_axis=1, tiled=True)
    partial_value = expert_rows(
        lax.all_gather(received.reshape(-1, model_width), "dp", axis=0, tiled=True),
        gate_w,
        up_w,
        down_w,
    )
    shares = lax.psum_scatter(
        partial_value.astype(jnp.bfloat16), "dp", scatter_dimension=0, tiled=True
    ).astype(jnp.float32)
    returned = lax.all_to_all(
        shares.reshape(experts, capacity, model_width).astype(jnp.bfloat16),
        "ep",
        split_axis=0,
        concat_axis=0,
        tiled=True,
    ).astype(jnp.float32)
    affinity = jax.nn.sigmoid(route_logits)
    weights = (ROUTE_SCALE * affinity / jnp.sum(affinity, axis=1, keepdims=True)).reshape(-1)
    own_target = own_flat[0] * capacity + own_slots[0]
    spread = jnp.where(
        own_target[:, None] == jnp.arange(experts * capacity, dtype=jnp.int32)[None, :],
        weights[:, None],
        0.0,
    )
    owners = (
        jnp.arange(tok_dev, dtype=jnp.int32)[:, None]
        == jnp.arange(per_block, dtype=jnp.int32)[None, :] // top_k
    ).astype(jnp.float32)
    combine = jnp.dot(owners, spread, precision=PRECISE)
    moe_output = jnp.dot(
        combine, returned.reshape(experts * capacity, model_width), precision=PRECISE
    ).astype(jnp.bfloat16)
    local_counts = own_counts[0].astype(jnp.float32)
    whole = lax.psum(local_counts, ("ep", "dp"))
    expert_count = lax.dynamic_slice_in_dim(whole, lax.axis_index("ep"), 1)
    mean_count = float(tok_dev * groups * top_k)
    expert_load = expert_count / mean_count
    return (moe_output, expert_load)


MESH = pl.DeviceIdType.MESH
RELAY_LAG = 1
X_LAG = 2
MM_LAG = 3
FAR_LAG = 3
FAR_X_LAG = 5
FAR_MM_LAG = 6
HALF_LAG = 1
SUM_EARLY = 3
SUM_LAG = 3
MIX_LAG = 5
OUT_LAG = 7
OUT_NEAR = 5
NEAR_AHEAD = 3
RAW_AHEAD = 1


def chunk_count(width):
    for count in (7, 7, 8, 4, 2):
        if width % (count * 128) == 0:
            return count
    return 1


def remote(src, dst, send, recv, ep, dp):
    return pltpu.make_async_remote_copy(
        src_ref=src,
        dst_ref=dst,
        send_sem=send,
        recv_sem=recv,
        device_id={"ep": ep, "dp": dp},
        device_id_type=MESH,
    )


def landed(ref, sem):
    pltpu.make_async_copy(ref, ref, sem).wait()


def wide(value):
    return value.astype(jnp.float32)


def fused_kernel(
    E, G, cap, nc, dc, mean_count,
    routes_hbm, logits_hbm, tokens_hbm, wg_hbm, wu_hbm, wd_hbm,
    out, load,
    routes, logits, tokens, far_routes, far_logits, far_tokens,
    wgu, wd, picker, combine, slots, rows, acc_g, acc_u, hidden, part,
    a_recv, b_send, b_recv, r_send, r_recv, p_send, p_recv, out_v, load_v,
    cnt_send, cnt_recv, dcnt_send, dcnt_recv,
    in_sem, w_sem, d_sem, t_send, t_recv, m_send, m_recv, s_send, s_recv, x_send, x_recv, c_send, c_recv,
    ra_send, ra_recv, rb_send, rb_recv, rr_send, rr_recv, p_sent, p_got,
    n_send, n_recv, nd_send, nd_recv, o_sem, l_sem,
):
    me = lax.axis_index("ep")
    dp = lax.axis_index("dp")
    hi = dp // 2
    lo = dp % 2
    px = (1 - hi) * 2 + lo
    pc = hi * 2 + (1 - lo)
    diagonal = (1 - hi) * 2 + (1 - lo)
    H = E // 2
    base = (me // H) * H
    mine = me - base
    mirror = lax.rem(me + H, E)
    top, tok = routes_hbm.shape
    n_slots = H * cap
    n_rows = G * n_slots

    def loop(lower, upper, body):
        def step(k, carry):
            body(k)
            return carry

        lax.fori_loop(lower, upper, step, 0)

    others = [jnp.where(mine + k >= H, mine + k - H, mine + k) for k in range(1, H)]

    def peers(body):
        for m in others:
            body(m)

    def ranked(body):
        for k, m in enumerate(others):
            body(k + 1, m)

    def everyone(body):
        loop(1, E, lambda k: body(lax.rem(me + k, E)))

    barrier = pltpu.get_barrier_semaphore()

    def greet(ep, who):
        pl.semaphore_signal(
            barrier, inc=1, device_id={"ep": ep, "dp": who}, device_id_type=MESH)

    greet(mirror, dp)
    peers(lambda m: greet(base + m, dp))
    greet(me, px)
    greet(me, pc)

    def columns(c):
        return pl.ds(pl.multiple_of(c * dc, 128), dc)

    own_routes = pltpu.make_async_copy(routes_hbm, routes, in_sem.at[0])
    own_logits = pltpu.make_async_copy(logits_hbm, logits, in_sem.at[1])
    own_routes.start()
    own_logits.start()
    loop(0, nc, lambda c: pltpu.make_async_copy(
        tokens_hbm.at[:, columns(c)], tokens.at[c], in_sem.at[2]).start())

    def weight_copies(c):
        return (
            pltpu.make_async_copy(wg_hbm.at[0, columns(c)], wgu.at[0, c], w_sem.at[c]),
            pltpu.make_async_copy(wu_hbm.at[0, columns(c)], wgu.at[1, c], w_sem.at[c]),
            pltpu.make_async_copy(wd_hbm.at[0, :, columns(c)], wd.at[c], d_sem),
        )

    def start_weights(c):
        copies = weight_copies(c)
        copies[0].start()
        copies[1].start()

    loop(0, nc, start_weights)
    loop(0, nc, lambda c: weight_copies(c)[2].start())

    def naming(table, first, amount):
        row = lax.broadcasted_iota(jnp.int32, (amount * cap, tok), 0)
        named = jnp.zeros((amount * cap, tok), jnp.float32)
        for k in range(top):
            named = named + jnp.where(table[k:k + 1, :] == first + row // cap, 1.0, 0.0)
        return row, named

    def placing(table):
        row, named = naming(table, base, H)
        earlier = jnp.where(
            lax.broadcasted_iota(jnp.int32, (tok, tok), 0)
            < lax.broadcasted_iota(jnp.int32, (tok, tok), 1), 1.0, 0.0)
        before = jnp.dot(named, earlier, preferred_element_type=jnp.float32)
        return row, named, before == (row % cap).astype(jnp.float32)

    def choose(table, h):
        _, named, placed = placing(table)
        picker[h] = jnp.where(placed, named, 0.0).astype(jnp.bfloat16)

    def weigh(table, scores, h):
        row, _, placed = placing(table)
        affinity = jax.nn.sigmoid(scores[...])
        weights = ROUTE_SCALE * affinity / jnp.sum(affinity, axis=0, keepdims=True)
        spread = jnp.zeros((n_slots, tok), jnp.float32)
        for k in range(top):
            hit = table[k:k + 1, :] == base + row // cap
            spread = spread + jnp.where(hit, weights[k:k + 1, :], 0.0)
        spread = jnp.where(placed, spread, 0.0)
        coarse = spread.astype(jnp.bfloat16)
        rest = spread - wide(coarse)
        middle = rest.astype(jnp.bfloat16)
        fine = (rest - wide(middle)).astype(jnp.bfloat16)
        same = jnp.where(
            lax.broadcasted_iota(jnp.int32, (tok, tok), 0)
            == lax.broadcasted_iota(jnp.int32, (tok, tok), 1), 1.0, 0.0).astype(jnp.bfloat16)
        for i, piece in enumerate((coarse, middle, fine)):
            turned = lax.dot_general(
                same, piece, (((1,), (1,)), ((), ())), preferred_element_type=jnp.float32)
            combine[h, i * tok:(i + 1) * tok] = turned.astype(jnp.bfloat16)

    def pack(source, c, h):
        filled = jnp.dot(picker[h], source[c], preferred_element_type=jnp.float32)
        slots[c, h] = filled.reshape(H, cap, dc).astype(jnp.bfloat16)
        rows[c, h, dp, 0] = slots[c, h, mine]
        across(c, h, slice(0, 1)).start()

    def weighted(c, h):
        got = wide(r_recv[c, h]).reshape(n_slots, dc).astype(jnp.bfloat16)
        mixed = jnp.dot(combine[h], got, preferred_element_type=jnp.float32)
        return mixed[0:tok] + mixed[tok:2 * tok] + mixed[2 * tok:3 * tok]

    def slot_send(c, h, k, m):
        return remote(slots.at[c, h, m], rows.at[c, h, dp, H - k],
                      s_send, s_recv.at[c, h], base + m, dp)

    def raw(c):
        return remote(tokens.at[c], far_tokens.at[c], t_send, t_recv.at[c], mirror, dp)

    def notes():
        return (
            remote(routes, far_routes, m_send.at[0], m_recv.at[0], mirror, dp),
            remote(logits, far_logits, m_send.at[1], m_recv.at[1], mirror, dp),
        )

    def across(c, h, places):
        block = rows.at[c, h, dp, places]
        return remote(block, block, x_send, x_recv.at[c, h], me, px)

    def beside(c, h, who):
        return remote(rows.at[c, h, who], rows.at[c, h, who], c_send, c_recv.at[c, h], me, pc)

    def half(c, h, side):
        return remote(part.at[c, h, side * 2 + (1 - lo)], a_recv.at[c, h, side],
                      ra_send, ra_recv.at[c, h], me, pc)

    def quarter(c, h):
        return remote(b_send.at[c, h], b_recv.at[c, h], rb_send, rb_recv.at[c, h], me, px)

    def back(c, h, k, m):
        return remote(r_send.at[c, h, k], r_recv.at[c, h, mine],
                      rr_send, rr_recv.at[c, h], base + m, dp)

    def share(c):
        return remote(p_send.at[c], p_recv.at[c], p_sent, p_got.at[c], mirror, dp)

    def counts(e):
        return remote(cnt_send.at[e], cnt_recv.at[me], n_send, n_recv, e, dp)

    own_routes.wait()
    choose(routes, 0)
    own_logits.wait()
    landed(tokens, in_sem.at[2])
    pl.semaphore_wait(barrier, H + 2)
    for note in notes():
        note.start()

    def offer(c):
        pack(tokens, c, 0)
        ranked(lambda k, m: slot_send(c, 0, k, m).start())

    near_ahead = min(NEAR_AHEAD, nc)
    raw_ahead = min(RAW_AHEAD, nc)

    def dispatch(c):
        offer(c)
        ratio = near_ahead // raw_ahead

        @pl.when(c % ratio == ratio - 1)
        def _():
            raw(c // ratio).start()

    loop(0, near_ahead, dispatch)
    acc_g[...] = jnp.zeros_like(acc_g)
    acc_u[...] = jnp.zeros_like(acc_u)

    near_start = MM_LAG + nc
    far_start = FAR_MM_LAG + nc
    early = far_start - near_start
    n_items = 2 * nc
    out_start = max(far_start + OUT_LAG, far_start + nc - early + OUT_NEAR)

    def stage(s, lag, amount, body):
        @pl.when((s >= lag) & (s < lag + amount))
        def _():
            body(s - lag)

    def returning(s, lag, early_lag, body):
        a, b = s - early_lag, s - lag
        first = (a >= near_start) & (a < near_start + early)
        later = (b >= far_start) & (b < far_start + n_items - early)

        @pl.when(first | later)
        def _():
            i = jnp.where(first, a - near_start, b - far_start + early)
            far = (i >= early) & (i < early + nc)
            h = jnp.where(far, 1, 0)
            c = jnp.where(i < early, i, jnp.where(far, i - early, i - nc))
            body(h, c)

    def near_in(c):
        landed(rows.at[c, 0, dp, 1:H], s_recv.at[c, 0])
        across(c, 0, slice(1, H)).start()
        beside(c, 0, dp).start()

    def relay(c):
        @pl.when(c == 0)
        def _():
            for note in notes():
                note.wait_recv()
            choose(far_routes, 1)

        landed(far_tokens.at[c], t_recv.at[c])
        pack(far_tokens, c, 1)
        ranked(lambda k, m: slot_send(c, 1, k, m).start())

    def far_in(c):
        landed(rows.at[c, 1, dp, 1:H], s_recv.at[c, 1])
        across(c, 1, slice(1, H)).start()
        beside(c, 1, dp).start()

    def crossed(c, h):
        landed(rows.at[c, h, dp], x_recv.at[c, h])
        beside(c, h, px).start()

    def expand(c, h):

        if h == 0:
            landed(wgu.at[:, c], w_sem.at[c])

        landed(rows.at[c, h, 0:2], c_recv.at[c, h])
        x = wide(rows[c, h]).reshape(n_rows, dc).astype(jnp.bfloat16)
        acc_g[h] += jnp.dot(x, wgu[0, c], preferred_element_type=jnp.float32)
        acc_u[h] += jnp.dot(x, wgu[1, c], preferred_element_type=jnp.float32)

        @pl.when(c == nc - 1)
        def _():
            gate = acc_g[h]
            hidden[h] = (gate / (1.0 + jnp.exp(-gate)) * acc_u[h]).astype(jnp.bfloat16)

    def contract(h, c):
        p = jnp.dot(hidden[h], wd[c], preferred_element_type=jnp.float32)
        part[c, h] = p.reshape(G, H, cap, dc).astype(jnp.bfloat16)
        half(c, h, 1 - hi).start()
        half(c, h, hi).start()

    def pair(h, c):
        landed(a_recv.at[c, h], ra_recv.at[c, h])
        total = wide(part[c, h, px]) + wide(a_recv[c, h, 1 - hi])
        b_send[c, h] = total.astype(jnp.bfloat16)
        quarter(c, h).start()

    def whole(h, c):
        landed(b_recv.at[c, h], rb_recv.at[c, h])
        total = wide(part[c, h, dp]) + wide(a_recv[c, h, hi]) + wide(b_recv[c, h])
        r_send[c, h] = total.astype(jnp.bfloat16)
        ranked(lambda k, m: back(c, h, k, m).start())
        r_recv[c, h, mine] = r_send[c, h, 0]

    def mix(c):
        landed(r_recv.at[c, 1, 0:H - 1], rr_recv.at[c, 1])
        p_send[c] = weighted(c, 1).astype(jnp.bfloat16)
        share(c).start()

    def finish(c):
        landed(r_recv.at[c, 0, 0:H - 1], rr_recv.at[c, 0])
        landed(p_recv.at[c], p_got.at[c])
        out_v[c] = (weighted(c, 0) + wide(p_recv[c])).astype(jnp.bfloat16)
        pltpu.make_async_copy(out_v.at[c], out.at[:, columns(c)], o_sem).start()

    def tally(_):
        _, named = naming(routes, 0, E)
        counted = jnp.sum(named, axis=1, keepdims=True)
        cnt_send[...] = jnp.broadcast_to(counted, (E * cap, 128)).reshape(E, cap, 128)
        cnt_recv[me] = cnt_send[me]
        everyone(lambda e: counts(e).start())

    def gather_counts(_):
        landed(cnt_recv.at[0:E - 1], n_recv)
        total = cnt_recv[0]
        for e in range(1, E):
            total = total + cnt_recv[e]
        dcnt_send[...] = total
        for i in range(1, G):
            remote(dcnt_send, dcnt_recv.at[i - 1], nd_send, nd_recv, me, lax.rem(dp + i, G)).start()

    def loads(_):
        landed(dcnt_recv, nd_recv)
        total = dcnt_send[...]
        for i in range(G - 1):
            total = total + dcnt_recv[i]
        load_v[...] = total[0:1, :] / mean_count
        pltpu.make_async_copy(load_v, load, l_sem).start()

    def weights_of(_):
        weigh(routes, logits, 0)
        weigh(far_routes, far_logits, 1)
        landed(wd, d_sem)

    def main(s):
        stage(s, 0, nc - near_ahead, lambda c: offer(c + near_ahead))
        stage(s, 0, nc - raw_ahead, lambda c: raw(c + raw_ahead).start())
        stage(s, 0, nc, near_in)
        stage(s, RELAY_LAG, nc, relay)
        stage(s, X_LAG, nc, lambda c: crossed(c, 0))
        stage(s, FAR_LAG, nc, far_in)
        stage(s, nc + 2, 1, weights_of)
        stage(s, MM_LAG, nc, lambda c: expand(c, 0))
        stage(s, FAR_X_LAG, nc, lambda c: crossed(c, 1))
        stage(s, FAR_MM_LAG, nc, lambda c: expand(c, 1))
        returning(s, HALF_LAG, HALF_LAG, pair)
        returning(s, 0, 0, contract)
        stage(s, near_start, 1, tally)
        stage(s, far_start + HALF_LAG, 1, gather_counts)
        stage(s, far_start + SUM_LAG + 2, 1, loads)
        returning(s, SUM_LAG, SUM_EARLY, whole)
        stage(s, far_start + MIX_LAG, nc, mix)
        stage(s, out_start, nc, finish)

    loop(0, out_start + nc, main)

    landed(cnt_recv.at[0:E - 1], n_send)
    landed(dcnt_recv, nd_send)
    for note in notes():
        note.wait_send()
    landed(tokens, t_send)
    landed(slots.at[:, :, 0:H - 1], s_send)
    landed(b_send, x_send)
    landed(a_recv, c_send)
    landed(a_recv, ra_send)
    landed(b_send, rb_send)
    landed(r_send.at[:, :, 1:H], rr_send)
    landed(p_send, p_sent)
    pltpu.make_async_copy(load_v, load, l_sem).wait()
    landed(out_v, o_sem)


def fused_device(tokens, routes, route_logits, gate_weight, up_weight, down_weight):
    tok_dev, top_k = routes.shape
    width = tokens.shape[1]
    units = gate_weight.shape[2]
    E = lax.axis_size("ep")
    G = lax.axis_size("dp")
    H = E // 2
    cap = min(tok_dev // 2, 2 * tok_dev * top_k // E)
    nc = chunk_count(width)
    dc = width // nc
    bf, f32 = jnp.bfloat16, jnp.float32
    dma = pltpu.SemaphoreType.DMA
    anywhere = pl.BlockSpec(memory_space=pl.ANY)
    rows = G * H * cap
    moe_output, load = pl.pallas_call(
        functools.partial(fused_kernel, E, G, cap, nc, dc, float(tok_dev * G * top_k)),
        out_shape=(
            jax.ShapeDtypeStruct((tok_dev, width), bf),
            jax.ShapeDtypeStruct((1, 128), f32),
        ),
        in_specs=[anywhere] * 6,
        out_specs=(anywhere, anywhere),
        scratch_shapes=[
            pltpu.VMEM((top_k, tok_dev), jnp.int32),
            pltpu.VMEM((top_k, tok_dev), f32),
            pltpu.VMEM((nc, tok_dev, dc), bf),
            pltpu.VMEM((top_k, tok_dev), jnp.int32),
            pltpu.VMEM((top_k, tok_dev), f32),
            pltpu.VMEM((nc, tok_dev, dc), bf),
            pltpu.VMEM((2, nc, dc, units), bf),
            pltpu.VMEM((nc, units, dc), bf),
            pltpu.VMEM((2, H * cap, tok_dev), bf),
            pltpu.VMEM((2, 3 * tok_dev, H * cap), bf),
            pltpu.VMEM((nc, 2, H, cap, dc), bf),
            pltpu.VMEM((nc, 2, G, H, cap, dc), bf),
            pltpu.VMEM((2, rows, units), f32),
            pltpu.VMEM((2, rows, units), f32),
            pltpu.VMEM((2, rows, units), bf),
            pltpu.VMEM((nc, 2, G, H, cap, dc), bf),
            pltpu.VMEM((nc, 2, 2, H, cap, dc), bf),
            pltpu.VMEM((nc, 2, H, cap, dc), bf),
            pltpu.VMEM((nc, 2, H, cap, dc), bf),
            pltpu.VMEM((nc, 2, H, cap, dc), bf),
            pltpu.VMEM((nc, 2, H, cap, dc), bf),
            pltpu.VMEM((nc, tok_dev, dc), bf),
            pltpu.VMEM((nc, tok_dev, dc), bf),
            pltpu.VMEM((nc, tok_dev, dc), bf),
            pltpu.VMEM((1, 128), f32),
            pltpu.VMEM((E, cap, 128), f32),
            pltpu.VMEM((E, cap, 128), f32),
            pltpu.VMEM((cap, 128), f32),
            pltpu.VMEM((G - 1, cap, 128), f32),
            dma((3,)), dma((nc,)), dma,
            dma, dma((nc,)),
            dma((2,)), dma((2,)),
            dma, dma((nc, 2)),
            dma, dma((nc, 2)),
            dma, dma((nc, 2)),
            dma, dma((nc, 2)),
            dma, dma((nc, 2)),
            dma, dma((nc, 2)),
            dma, dma((nc,)),
            dma, dma,
            dma, dma,
            dma, dma,
        ],
        compiler_params=pltpu.CompilerParams(
            collective_id=0, has_side_effects=True, vmem_limit_bytes=60 * 2**20
        ),
    )(routes.T, route_logits.T, tokens, gate_weight, up_weight, down_weight)
    return moe_output, load[0, :1]


def fits(mesh):
    return mesh.shape["dp"] == 4 and mesh.shape["ep"] in (4, 8)


def solution(mesh):
    body = fused_device if fits(mesh) else on_device
    return jax.shard_map(
        body,
        mesh=mesh,
        in_specs=(
            P(("ep", "dp"), None),
            P(("ep", "dp"), None),
            P(("ep", "dp"), None),
            P("ep", None, "dp"),
            P("ep", None, "dp"),
            P("ep", "dp", None),
        ),
        out_specs=(P(("ep", "dp"), None), P("ep")),
        check_vma=False,
    )
```

```python
import functools

import jax
import jax.numpy as jnp
from jax import lax
from jax.experimental import pallas as pl
from jax.experimental.pallas import tpu as pltpu
from jax.sharding import PartitionSpec as P

ROUTE_SCALE = 2.5
PRECISE = lax.Precision.HIGHEST


def assignment_slots(flat_routes, experts):
    labels = jnp.arange(experts, dtype=jnp.int32)
    onehot = (flat_routes[:, :, None] == labels[None, None, :]).astype(jnp.int32)
    before = jnp.cumsum(onehot, axis=1) - onehot
    return (jnp.sum(before * onehot, axis=2), jnp.sum(onehot, axis=1))


def pack(members, flat_routes, slot_ids, experts, capacity, top_k):
    blocks, per_block = flat_routes.shape
    tok_dev = per_block // top_k
    member = jnp.arange(blocks, dtype=jnp.int32)[:, None]
    target = ((member * experts + flat_routes) * capacity + slot_ids).reshape(-1)
    source = (member * tok_dev + jnp.arange(per_block, dtype=jnp.int32)[None, :] // top_k).reshape(
        -1
    )
    placing = (
        jnp.arange(blocks * experts * capacity, dtype=jnp.int32)[:, None] == target[None, :]
    ).astype(jnp.bfloat16)
    owners = (source[:, None] == jnp.arange(blocks * tok_dev, dtype=jnp.int32)[None, :]).astype(
        jnp.bfloat16
    )
    picker = jnp.dot(placing, owners, preferred_element_type=jnp.float32).astype(jnp.bfloat16)
    filled = jnp.dot(picker, members, preferred_element_type=jnp.float32).astype(jnp.bfloat16)
    return filled.reshape(blocks, experts, capacity, members.shape[1])


def expert_rows(row_block, gate_w, up_w, down_w):
    gate_act = jnp.dot(row_block, gate_w, preferred_element_type=jnp.float32)
    up_act = jnp.dot(row_block, up_w, preferred_element_type=jnp.float32)
    hidden = (jax.nn.silu(gate_act) * up_act).astype(jnp.bfloat16)
    return jnp.dot(hidden, down_w, preferred_element_type=jnp.float32)


def on_device(tokens, routes, route_logits, gate_weight, up_weight, down_weight):
    tok_dev, top_k = routes.shape
    model_width = tokens.shape[1]
    experts = lax.axis_size("ep")
    groups = lax.axis_size("dp")
    capacity = min(tok_dev // 2, 2 * tok_dev * top_k // experts)
    per_block = tok_dev * top_k
    gate_w = gate_weight[0]
    up_w = up_weight[0]
    down_w = down_weight[0]
    own_flat = routes.reshape(1, per_block)
    own_slots, own_counts = assignment_slots(own_flat, experts)
    buffer = pack(tokens, own_flat, own_slots, experts, capacity, top_k)
    received = lax.all_to_all(buffer, "ep", split_axis=1, concat_axis=1, tiled=True)
    partial_value = expert_rows(
        lax.all_gather(received.reshape(-1, model_width), "dp", axis=0, tiled=True),
        gate_w,
        up_w,
        down_w,
    )
    shares = lax.psum_scatter(
        partial_value.astype(jnp.bfloat16), "dp", scatter_dimension=0, tiled=True
    ).astype(jnp.float32)
    returned = lax.all_to_all(
        shares.reshape(experts, capacity, model_width).astype(jnp.bfloat16),
        "ep",
        split_axis=0,
        concat_axis=0,
        tiled=True,
    ).astype(jnp.float32)
    affinity = jax.nn.sigmoid(route_logits)
    weights = (ROUTE_SCALE * affinity / jnp.sum(affinity, axis=1, keepdims=True)).reshape(-1)
    own_target = own_flat[0] * capacity + own_slots[0]
    spread = jnp.where(
        own_target[:, None] == jnp.arange(experts * capacity, dtype=jnp.int32)[None, :],
        weights[:, None],
        0.0,
    )
    owners = (
        jnp.arange(tok_dev, dtype=jnp.int32)[:, None]
        == jnp.arange(per_block, dtype=jnp.int32)[None, :] // top_k
    ).astype(jnp.float32)
    combine = jnp.dot(owners, spread, precision=PRECISE)
    moe_output = jnp.dot(
        combine, returned.reshape(experts * capacity, model_width), precision=PRECISE
    ).astype(jnp.bfloat16)
    local_counts = own_counts[0].astype(jnp.float32)
    whole = lax.psum(local_counts, ("ep", "dp"))
    expert_count = lax.dynamic_slice_in_dim(whole, lax.axis_index("ep"), 1)
    mean_count = float(tok_dev * groups * top_k)
    expert_load = expert_count / mean_count
    return (moe_output, expert_load)


MESH = pl.DeviceIdType.MESH
RELAY_LAG = 1
NEAR_LAG = 0
X_LAG = 2
MM_LAG = 3
FAR_LAG = 3
FAR_X_LAG = 5
FAR_MM_LAG = 6
HALF_LAG = 0
SUM_EARLY = 3
SUM_LAG = 3
MIX_LAG = 5
OUT_LAG = 7
OUT_NEAR = 5
NEAR_AHEAD = 3
RAW_AHEAD = 1


def chunk_count(width):
    for count in (7, 7, 8, 4, 2):
        if width % (count * 128) == 0:
            return count
    return 1


def remote(src, dst, send, recv, ep, dp):
    return pltpu.make_async_remote_copy(
        src_ref=src,
        dst_ref=dst,
        send_sem=send,
        recv_sem=recv,
        device_id={"ep": ep, "dp": dp},
        device_id_type=MESH,
    )


def landed(ref, sem):
    pltpu.make_async_copy(ref, ref, sem).wait()


def wide(value):
    return value.astype(jnp.float32)


def fused_kernel(
    E, G, cap, nc, dc, mean_count,
    routes_hbm, logits_hbm, tokens_hbm, wg_hbm, wu_hbm, wd_hbm,
    out, load,
    routes, logits, tokens, far_routes, far_logits, far_tokens,
    wgu, wd, picker, combine, slots, rows, acc_g, acc_u, hidden, part,
    a_recv, b_send, b_recv, r_send, r_recv, p_send, p_recv, out_v, load_v,
    cnt_send, cnt_recv, dcnt_send, dcnt_recv,
    in_sem, w_sem, d_sem, t_send, t_recv, m_send, m_recv, s_send, s_recv, y_recv, x_send, x_recv, c_send, c_recv,
    ra_send, ra_recv, rb_send, rb_recv, rr_send, rr_recv, p_sent, p_got,
    n_send, n_recv, nd_send, nd_recv, o_sem, l_sem,
):
    me = lax.axis_index("ep")
    dp = lax.axis_index("dp")
    hi = dp // 2
    lo = dp % 2
    px = (1 - hi) * 2 + lo
    pc = hi * 2 + (1 - lo)
    diagonal = (1 - hi) * 2 + (1 - lo)
    H = E // 2
    base = (me // H) * H
    mine = me - base
    mirror = lax.rem(me + H, E)
    top, tok = routes_hbm.shape
    n_slots = H * cap
    n_rows = G * n_slots

    def loop(lower, upper, body):
        def step(k, carry):
            body(k)
            return carry

        lax.fori_loop(lower, upper, step, 0)

    side, level = mine % 2, mine // 2
    members = (
        mine,
        level * 2 + (1 - side),
        (1 - level) * 2 + side,
        (1 - level) * 2 + (1 - side),
    )

    def everyone(body):
        loop(1, E, lambda k: body(lax.rem(me + k, E)))

    barrier = pltpu.get_barrier_semaphore()

    def greet(ep, who):
        pl.semaphore_signal(
            barrier, inc=1, device_id={"ep": ep, "dp": who}, device_id_type=MESH)

    greet(mirror, dp)
    for m in members[1:]:
        greet(base + m, dp)
    greet(me, px)
    greet(me, pc)

    def columns(c):
        return pl.ds(pl.multiple_of(c * dc, 128), dc)

    own_routes = pltpu.make_async_copy(routes_hbm, routes, in_sem.at[0])
    own_logits = pltpu.make_async_copy(logits_hbm, logits, in_sem.at[1])
    own_routes.start()
    own_logits.start()
    loop(0, nc, lambda c: pltpu.make_async_copy(
        tokens_hbm.at[:, columns(c)], tokens.at[c], in_sem.at[2]).start())

    def weight_copies(c):
        return (
            pltpu.make_async_copy(wg_hbm.at[0, columns(c)], wgu.at[0, c], w_sem.at[c]),
            pltpu.make_async_copy(wu_hbm.at[0, columns(c)], wgu.at[1, c], w_sem.at[c]),
            pltpu.make_async_copy(wd_hbm.at[0, :, columns(c)], wd.at[c], d_sem),
        )

    def start_weights(c):
        copies = weight_copies(c)
        copies[0].start()
        copies[1].start()

    loop(0, nc, start_weights)
    loop(0, nc, lambda c: weight_copies(c)[2].start())

    def naming(table, first, amount):
        row = lax.broadcasted_iota(jnp.int32, (amount * cap, tok), 0)
        named = jnp.zeros((amount * cap, tok), jnp.float32)
        for k in range(top):
            named = named + jnp.where(table[k:k + 1, :] == first + row // cap, 1.0, 0.0)
        return row, named

    def placing(table):
        row, named = naming(table, base, H)
        earlier = jnp.where(
            lax.broadcasted_iota(jnp.int32, (tok, tok), 0)
            < lax.broadcasted_iota(jnp.int32, (tok, tok), 1), 1.0, 0.0)
        before = jnp.dot(named, earlier, preferred_element_type=jnp.float32)
        return row, named, before == (row % cap).astype(jnp.float32)

    def choose(table, h):
        _, named, placed = placing(table)
        picker[h] = jnp.where(placed, named, 0.0).astype(jnp.bfloat16)

    def weigh(table, scores, h):
        row, _, placed = placing(table)
        affinity = jax.nn.sigmoid(scores[...])
        weights = ROUTE_SCALE * affinity / jnp.sum(affinity, axis=0, keepdims=True)
        spread = jnp.zeros((n_slots, tok), jnp.float32)
        for k in range(top):
            hit = table[k:k + 1, :] == base + row // cap
            spread = spread + jnp.where(hit, weights[k:k + 1, :], 0.0)
        spread = jnp.where(placed, spread, 0.0)
        coarse = spread.astype(jnp.bfloat16)
        rest = spread - wide(coarse)
        middle = rest.astype(jnp.bfloat16)
        fine = (rest - wide(middle)).astype(jnp.bfloat16)
        same = jnp.where(
            lax.broadcasted_iota(jnp.int32, (tok, tok), 0)
            == lax.broadcasted_iota(jnp.int32, (tok, tok), 1), 1.0, 0.0).astype(jnp.bfloat16)
        for i, piece in enumerate((coarse, middle, fine)):
            turned = lax.dot_general(
                same, piece, (((1,), (1,)), ((), ())), preferred_element_type=jnp.float32)
            combine[h, i * tok:(i + 1) * tok] = turned.astype(jnp.bfloat16)

    def pack(source, c, h):
        filled = jnp.dot(picker[h], source[c], preferred_element_type=jnp.float32)
        slots[c, h] = filled.reshape(H, cap, dc).astype(jnp.bfloat16)
        rows[c, h, dp, 0] = slots[c, h, mine]
        across(c, h, slice(0, 1)).start()

    def weighted(c, h):
        got = wide(r_recv[c, h]).reshape(n_slots, dc).astype(jnp.bfloat16)
        mixed = jnp.dot(combine[h], got, preferred_element_type=jnp.float32)
        return mixed[0:tok] + mixed[tok:2 * tok] + mixed[2 * tok:3 * tok]

    def slot_send(c, h, k):
        arrived = y_recv.at[c] if (h, k) == (0, 1) else s_recv.at[c, h]
        return remote(slots.at[c, h, members[k]], rows.at[c, h, dp, k],
                      s_send, arrived, base + members[k], dp)

    def raw(c):
        return remote(tokens.at[c], far_tokens.at[c], t_send, t_recv.at[c], mirror, dp)

    def notes():
        return (
            remote(routes, far_routes, m_send.at[0], m_recv.at[0], mirror, dp),
            remote(logits, far_logits, m_send.at[1], m_recv.at[1], mirror, dp),
        )

    def across(c, h, places):
        block = rows.at[c, h, dp, places]
        return remote(block, block, x_send, x_recv.at[c, h], me, px)

    def beside(c, h, who):
        return remote(rows.at[c, h, who], rows.at[c, h, who], c_send, c_recv.at[c, h], me, pc)

    def half(c, h, side):
        return remote(part.at[c, h, side * 2 + (1 - lo)], a_recv.at[c, h, side],
                      ra_send, ra_recv.at[c, h], me, pc)

    def quarter(c, h):
        return remote(b_send.at[c, h], b_recv.at[c, h], rb_send, rb_recv.at[c, h], me, px)

    def back(c, h, k):
        return remote(r_send.at[c, h, k], r_recv.at[c, h, mine],
                      rr_send, rr_recv.at[c, h], base + members[k], dp)

    def share(c):
        return remote(p_send.at[c], p_recv.at[c], p_sent, p_got.at[c], mirror, dp)

    def counts(e):
        return remote(cnt_send.at[e], cnt_recv.at[me], n_send, n_recv, e, dp)

    own_routes.wait()
    choose(routes, 0)
    own_logits.wait()
    landed(tokens, in_sem.at[2])
    pl.semaphore_wait(barrier, H + 2)
    for note in notes():
        note.start()

    def ahead(c):
        slot_send(c, 0, 2).start()
        slot_send(c, 0, 3).start()

    near_ahead = min(NEAR_AHEAD, nc)
    raw_ahead = min(RAW_AHEAD, nc)

    def dispatch(c):
        pack(tokens, c, 0)
        slot_send(c, 0, 1).start()

        @pl.when(c < raw_ahead)
        def _():
            raw(c).start()

        @pl.when(c < near_ahead)
        def _():
            ahead(c)

    loop(0, nc, dispatch)
    acc_g[...] = jnp.zeros_like(acc_g)
    acc_u[...] = jnp.zeros_like(acc_u)

    near_start = MM_LAG + nc - 1
    far_start = FAR_MM_LAG + nc
    early = far_start - near_start
    n_items = 2 * nc
    out_start = max(far_start + OUT_LAG, far_start + nc - early + OUT_NEAR)

    def stage(s, lag, amount, body):
        @pl.when((s >= lag) & (s < lag + amount))
        def _():
            body(s - lag)

    def returning(s, lag, early_lag, body):
        a, b = s - early_lag, s - lag
        first = (a >= near_start) & (a < near_start + early)
        later = (b >= far_start) & (b < far_start + n_items - early)

        @pl.when(first | later)
        def _():
            i = jnp.where(first, a - near_start, b - far_start + early)
            far = (i >= early) & (i < early + nc)
            h = jnp.where(far, 1, 0)
            c = jnp.where(i < early, i, jnp.where(far, i - early, i - nc))
            body(h, c)

    def beside_in(c):
        landed(rows.at[c, 0, dp, 1], y_recv.at[c])
        across(c, 0, slice(1, 2)).start()

    def near_in(c):
        landed(rows.at[c, 0, dp, 2:H], s_recv.at[c, 0])
        across(c, 0, slice(2, H)).start()
        beside(c, 0, dp).start()

    def relay(c):
        @pl.when(c == 0)
        def _():
            for note in notes():
                note.wait_recv()
            choose(far_routes, 1)

        landed(far_tokens.at[c], t_recv.at[c])
        pack(far_tokens, c, 1)
        for k in range(1, H):
            slot_send(c, 1, k).start()

    def far_in(c):
        landed(rows.at[c, 1, dp, 1:H], s_recv.at[c, 1])
        across(c, 1, slice(1, H)).start()
        beside(c, 1, dp).start()

    def crossed(c, h):
        landed(rows.at[c, h, dp], x_recv.at[c, h])
        beside(c, h, px).start()

    def expand(c, h):

        if h == 0:
            landed(wgu.at[:, c], w_sem.at[c])

        landed(rows.at[c, h, 0:2], c_recv.at[c, h])
        x = wide(rows[c, h]).reshape(n_rows, dc).astype(jnp.bfloat16)
        acc_g[h] += jnp.dot(x, wgu[0, c], preferred_element_type=jnp.float32)
        acc_u[h] += jnp.dot(x, wgu[1, c], preferred_element_type=jnp.float32)

        @pl.when(c == nc - 1)
        def _():
            gate = acc_g[h]
            hidden[h] = (gate / (1.0 + jnp.exp(-gate)) * acc_u[h]).astype(jnp.bfloat16)

    def contract(h, c):
        p = jnp.dot(hidden[h], wd[c], preferred_element_type=jnp.float32)
        part[c, h] = p.reshape(G, H, cap, dc).astype(jnp.bfloat16)
        half(c, h, 1 - hi).start()
        half(c, h, hi).start()

    def pair(h, c):
        landed(a_recv.at[c, h], ra_recv.at[c, h])
        total = wide(part[c, h, px]) + wide(a_recv[c, h, 1 - hi])
        b_send[c, h] = total.astype(jnp.bfloat16)
        quarter(c, h).start()

    def whole(h, c):
        landed(b_recv.at[c, h], rb_recv.at[c, h])
        total = wide(part[c, h, dp]) + wide(a_recv[c, h, hi]) + wide(b_recv[c, h])
        r_send[c, h] = total.astype(jnp.bfloat16)
        for k in range(1, H):
            back(c, h, k).start()
        r_recv[c, h, mine] = r_send[c, h, 0]

    def mix(c):
        landed(r_recv.at[c, 1, 0:H - 1], rr_recv.at[c, 1])
        p_send[c] = weighted(c, 1).astype(jnp.bfloat16)
        share(c).start()

    def finish(c):
        landed(r_recv.at[c, 0, 0:H - 1], rr_recv.at[c, 0])
        landed(p_recv.at[c], p_got.at[c])
        out_v[c] = (weighted(c, 0) + wide(p_recv[c])).astype(jnp.bfloat16)
        pltpu.make_async_copy(out_v.at[c], out.at[:, columns(c)], o_sem).start()

    def tally(_):
        _, named = naming(routes, 0, E)
        counted = jnp.sum(named, axis=1, keepdims=True)
        cnt_send[...] = jnp.broadcast_to(counted, (E * cap, 128)).reshape(E, cap, 128)
        cnt_recv[me] = cnt_send[me]
        everyone(lambda e: counts(e).start())

    def gather_counts(_):
        landed(cnt_recv.at[0:E - 1], n_recv)
        total = cnt_recv[0]
        for e in range(1, E):
            total = total + cnt_recv[e]
        dcnt_send[...] = total
        for i in range(1, G):
            remote(dcnt_send, dcnt_recv.at[i - 1], nd_send, nd_recv, me, lax.rem(dp + i, G)).start()

    def loads(_):
        landed(dcnt_recv, nd_recv)
        total = dcnt_send[...]
        for i in range(G - 1):
            total = total + dcnt_recv[i]
        load_v[...] = total[0:1, :] / mean_count
        pltpu.make_async_copy(load_v, load, l_sem).start()

    def weights_of(_):
        weigh(routes, logits, 0)
        weigh(far_routes, far_logits, 1)
        landed(wd, d_sem)

    def main(s):
        stage(s, 0, nc - raw_ahead, lambda c: raw(c + raw_ahead).start())
        stage(s, 0, nc - near_ahead, lambda c: ahead(c + near_ahead))
        stage(s, 0, nc, beside_in)
        stage(s, NEAR_LAG, nc, near_in)
        stage(s, RELAY_LAG, nc, relay)
        stage(s, X_LAG, nc, lambda c: crossed(c, 0))
        stage(s, FAR_LAG, nc, far_in)
        stage(s, nc + 2, 1, weights_of)
        stage(s, MM_LAG, nc, lambda c: expand(c, 0))
        returning(s, 0, 0, contract)
        stage(s, near_start, 1, tally)
        stage(s, FAR_X_LAG, nc, lambda c: crossed(c, 1))
        stage(s, FAR_MM_LAG, nc, lambda c: expand(c, 1))
        returning(s, SUM_LAG, SUM_EARLY, whole)
        stage(s, far_start + 1, 1, gather_counts)
        stage(s, far_start + MIX_LAG, nc, mix)
        stage(s, far_start + SUM_LAG + 2, 1, loads)
        stage(s, out_start, nc, finish)
        returning(s, HALF_LAG, HALF_LAG, pair)

    loop(0, out_start + nc, main)

    landed(cnt_recv.at[0:E - 1], n_send)
    landed(dcnt_recv, nd_send)
    for note in notes():
        note.wait_send()
    landed(tokens, t_send)
    landed(slots.at[:, :, 0:H - 1], s_send)
    landed(b_send, x_send)
    landed(a_recv, c_send)
    landed(a_recv, ra_send)
    landed(b_send, rb_send)
    landed(r_send.at[:, :, 1:H], rr_send)
    landed(p_send, p_sent)
    pltpu.make_async_copy(load_v, load, l_sem).wait()
    landed(out_v, o_sem)


def fused_device(tokens, routes, route_logits, gate_weight, up_weight, down_weight):
    tok_dev, top_k = routes.shape
    width = tokens.shape[1]
    units = gate_weight.shape[2]
    E = lax.axis_size("ep")
    G = lax.axis_size("dp")
    H = E // 2
    cap = min(tok_dev // 2, 2 * tok_dev * top_k // E)
    nc = chunk_count(width)
    dc = width // nc
    bf, f32 = jnp.bfloat16, jnp.float32
    dma = pltpu.SemaphoreType.DMA
    anywhere = pl.BlockSpec(memory_space=pl.ANY)
    rows = G * H * cap
    moe_output, load = pl.pallas_call(
        functools.partial(fused_kernel, E, G, cap, nc, dc, float(tok_dev * G * top_k)),
        out_shape=(
            jax.ShapeDtypeStruct((tok_dev, width), bf),
            jax.ShapeDtypeStruct((1, 128), f32),
        ),
        in_specs=[anywhere] * 6,
        out_specs=(anywhere, anywhere),
        scratch_shapes=[
            pltpu.VMEM((top_k, tok_dev), jnp.int32),
            pltpu.VMEM((top_k, tok_dev), f32),
            pltpu.VMEM((nc, tok_dev, dc), bf),
            pltpu.VMEM((top_k, tok_dev), jnp.int32),
            pltpu.VMEM((top_k, tok_dev), f32),
            pltpu.VMEM((nc, tok_dev, dc), bf),
            pltpu.VMEM((2, nc, dc, units), bf),
            pltpu.VMEM((nc, units, dc), bf),
            pltpu.VMEM((2, H * cap, tok_dev), bf),
            pltpu.VMEM((2, 3 * tok_dev, H * cap), bf),
            pltpu.VMEM((nc, 2, H, cap, dc), bf),
            pltpu.VMEM((nc, 2, G, H, cap, dc), bf),
            pltpu.VMEM((2, rows, units), f32),
            pltpu.VMEM((2, rows, units), f32),
            pltpu.VMEM((2, rows, units), bf),
            pltpu.VMEM((nc, 2, G, H, cap, dc), bf),
            pltpu.VMEM((nc, 2, 2, H, cap, dc), bf),
            pltpu.VMEM((nc, 2, H, cap, dc), bf),
            pltpu.VMEM((nc, 2, H, cap, dc), bf),
            pltpu.VMEM((nc, 2, H, cap, dc), bf),
            pltpu.VMEM((nc, 2, H, cap, dc), bf),
            pltpu.VMEM((nc, tok_dev, dc), bf),
            pltpu.VMEM((nc, tok_dev, dc), bf),
            pltpu.VMEM((nc, tok_dev, dc), bf),
            pltpu.VMEM((1, 128), f32),
            pltpu.VMEM((E, cap, 128), f32),
            pltpu.VMEM((E, cap, 128), f32),
            pltpu.VMEM((cap, 128), f32),
            pltpu.VMEM((G - 1, cap, 128), f32),
            dma((3,)), dma((nc,)), dma,
            dma, dma((nc,)),
            dma((2,)), dma((2,)),
            dma, dma((nc, 2)), dma((nc,)),
            dma, dma((nc, 2)),
            dma, dma((nc, 2)),
            dma, dma((nc, 2)),
            dma, dma((nc, 2)),
            dma, dma((nc, 2)),
            dma, dma((nc,)),
            dma, dma,
            dma, dma,
            dma, dma,
        ],
        compiler_params=pltpu.CompilerParams(
            collective_id=0, has_side_effects=True, vmem_limit_bytes=60 * 2**20
        ),
    )(routes.T, route_logits.T, tokens, gate_weight, up_weight, down_weight)
    return moe_output, load[0, :1]


def fits(mesh):
    return mesh.shape["dp"] == 4 and mesh.shape["ep"] == 8


def solution(mesh):
    body = fused_device if fits(mesh) else on_device
    return jax.shard_map(
        body,
        mesh=mesh,
        in_specs=(
            P(("ep", "dp"), None),
            P(("ep", "dp"), None),
            P(("ep", "dp"), None),
            P("ep", None, "dp"),
            P("ep", None, "dp"),
            P("ep", "dp", None),
        ),
        out_specs=(P(("ep", "dp"), None), P("ep")),
        check_vma=False,
    )
```
